32 devices in a mesh: grp: 4 (over y, core), blk: 8 (over z, x).
Axes of the slice: x: 2, y: 2, z: 4, core: 2. Of those that a mesh axis runs over, the one named last changes fastest.
Arguments:
- embeds: bfloat16 [4, 8192, 1024], P('grp', 'blk')
- doc_ids: int32 [4, 8192], P('grp', 'blk'), may hold values from 0 to 8191, each once within a row
- prior_max: float32 [4, 8192], P('grp', 'blk'), may hold values from -0.2 to 0.6
- owned: bfloat16 [2048, 1024], P(('grp', 'blk')), may hold values from -6 to 6
- owned_ids: int32 [2048], P(('grp', 'blk')), may hold values from 0 to 2047, each once
- owner_dest: int32 [2048, 1], P(('grp', 'blk')), may hold values from 0 to 31; in each aligned block of 64 rows (0 to 63, 64 to 127, ...) at most 4 rows name the same one
Outputs:
- running_max: float32 [4, 8192], P('grp', 'blk')
- next_rows: bfloat16 [4096, 1024], P(('grp', 'blk'))
- next_ids: int32 [4096], P(('grp', 'blk'))
The draws below stay inside these ranges and needn't reach their ends.
Inputs may be any that keep to these rules, and one draw needn't show every extreme that they name: `owner_dest`: among the 64 rows of one device no target is named more than 4 times, a bound that some block reaches.
All inputs are finite; a program needn't handle non-finite values.
Results may differ from the reference program's by a relative error of at most 0.0016.
Values may be sent and summed in bfloat16 or wider, within the bound.
A program may use at most 64 MiB of HBM per device.

```python
import math
import jax
import jax.numpy as jnp
import numpy as np
from jax import lax

E = 1024
ROWS_DEV = 1024
CYCLE = 3
CAP = 4
CR = 8192
OWN_DEV = 64
TOTAL_OWN = 2048
SLOTS = 128
N_GRP = 4
N_BLK = 8
DEVICES = 32


def draw_embeds(key, part):
    keys = jax.random.split(jax.random.fold_in(key, 7), 4)
    nblk = CR // ROWS_DEV
    base = jax.random.normal(keys[0], (N_GRP, CR, E), jnp.float32)
    offset = jax.random.randint(keys[1], (N_GRP, CR), 0, CYCLE + 1)
    within = jax.random.randint(keys[2], (N_GRP, CR), 0, ROWS_DEV)
    blocks = jnp.arange(CR, dtype=jnp.int32)[None, :] // ROWS_DEV
    partner = (blocks - offset) % nblk * ROWS_DEV + within
    partner_rows = jnp.take_along_axis(base, partner[:, :, None], axis=1)
    weight = jnp.exp(jax.random.uniform(keys[3], (N_GRP, CR, 1), jnp.float32, jnp.log(0.3), jnp.log(3.0)))
    result = base + weight * partner_rows
    return result.astype(jnp.bfloat16)


def levels(own_key, shape, pieces, smallest, high):
    def one(dim, blocks):
        draws = jax.random.uniform(jax.random.fold_in(jax.random.fold_in(own_key, 6), dim), (blocks,), jnp.float32, smallest / len(pieces), high / len(pieces))
        return jnp.repeat(jnp.exp(draws), shape[dim] // blocks).reshape((-1,) + (1,) * (len(shape) - dim - 1))

    gain = one(*pieces[0])
    for cut in pieces[1:]:
        gain = gain * one(*cut)
    return gain


def deal_out(key, own, number, rows, number_of, top, limit, lean):
    order = jax.random.permutation(key, number_of)
    heavy_load, ordinary = load_shares(number_of, rows * top, limit, lean, True), load_shares(number_of, rows * top, limit, lean, False)
    places = jnp.arange(number_of)

    def named(sizes, turn):
        used = int((sizes > 0).sum())
        fixed = max(1, used // 4)
        moved = fixed + (places - fixed + turn * (used - fixed)) % max(1, number_of - fixed)
        return jnp.zeros((number_of,), jnp.int32).at[order[jnp.where(places < fixed, places, moved)]].set(jnp.asarray(sizes, jnp.int32))

    sizes = jnp.where(number % 4 == 0, named(heavy_load, number // 4), named(ordinary, number - number // 4 - 1))
    mixed = jax.random.permutation(jax.random.fold_in(own, 3), number_of)
    giver, taker = mixed[0:number_of // 2 * 2:2], mixed[1:number_of // 2 * 2:2]
    room = jnp.minimum(sizes[giver] - 1, limit - sizes[taker]) // 2
    room = jnp.where((giver == order[0]) | (taker == order[0]) | (sizes[taker] == 0), 0, jnp.maximum(room, 0))
    moved = jax.random.randint(jax.random.fold_in(own, 4), (number_of // 2,), 0, 1 << 20) % (room + 1)
    sizes = sizes.at[giver].add(-moved).at[taker].add(moved)
    items = jnp.searchsorted(jnp.cumsum(sizes), jnp.arange(rows * top), side="right").astype(jnp.int32)
    grid = items.reshape(top, rows).T
    grid = grid[jax.random.permutation(jax.random.fold_in(own, 1), rows)]
    turn = jax.random.randint(jax.random.fold_in(own, 2), (rows, 1), 0, top)
    return jnp.take_along_axis(grid, (jnp.arange(top)[None, :] + turn) % top, axis=1)


def load_shares(number_of, total, reach, skew, full):
    loads = [(1 << 20) // math.isqrt(standing ** skew) + 1 for standing in range(1, number_of + 1)]
    largest = reach if full else min(reach, max(-(-total // number_of), total * loads[0] // sum(loads)))
    least = 1 if total - largest >= number_of - 1 else 0
    given, surplus = [largest] + [least] * (number_of - 1), total - largest - least * (number_of - 1)
    while surplus > 0:
        free = [i for i in range(1, number_of) if given[i] < largest] or [i for i in range(1, number_of) if given[i] < reach]
        mass, left = sum([loads[i] for i in free]), surplus
        for i in free:
            addition = min(reach - given[i], max(1, left * loads[i] // mass), surplus)
            given[i] = given[i] + addition
            surplus = surplus - addition
    return np.array(given)


def noise(key, extent, spread, bound, cuts=(), held_as=jnp.bfloat16):
    gain = levels(key, extent, cuts, -0.22, 0.18) if cuts else 1.0
    array = jax.random.normal(key, extent, jnp.float32) * spread * gain
    return jnp.minimum(jnp.maximum(array, -bound), bound).astype(held_as)


def setup_inputs(seed: int = 0) -> dict:
    key_list = jax.random.split(jax.random.key(seed), 7)
    embeds = draw_embeds(jax.random.fold_in(key_list[6], 71), 0)
    doc_ids = jax.vmap(lambda own: jax.random.permutation(own, CR))(jax.random.split(key_list[1], N_GRP)).reshape((N_GRP, CR)).astype(jnp.int32)
    prior_max = jnp.clip(-0.2 + 0.8 * jax.random.uniform(key_list[2], (N_GRP, CR), jnp.float32) ** levels(key_list[2], (N_GRP, CR), ((0, 4), (1, 8)), -0.2, 0.2), -0.2, 0.6)
    owned = noise(key_list[3], (TOTAL_OWN, E), 1.0, 6.0, ((0, 32),))
    owned_ids = jax.random.permutation(key_list[4], TOTAL_OWN).astype(jnp.int32)
    owner_dest_keys = jax.random.split(jax.random.fold_in(key_list[5], 1), TOTAL_OWN // OWN_DEV)
    owner_dest_turns = jax.random.permutation(jax.random.fold_in(key_list[5], 3), TOTAL_OWN // OWN_DEV)
    owner_dest = jax.vmap(lambda own, number: deal_out(jax.random.fold_in(key_list[5], 2), own, number, OWN_DEV, DEVICES, 1, CAP, 2))(owner_dest_keys, owner_dest_turns).reshape((TOTAL_OWN, 1))
    return {"embeds": embeds, "doc_ids": doc_ids, "prior_max": prior_max, "owned": owned, "owned_ids": owned_ids, "owner_dest": owner_dest}


def normalize(matrix):
    values = matrix.astype(jnp.float32)
    scale = lax.rsqrt(lax.optimization_barrier(jnp.sum(values * values, axis=-1, keepdims=True)) + 1e-06)
    return (values * scale).astype(jnp.bfloat16)

def tile_max(operands):
    row_normed, row_ids, col_normed, col_ids = operands
    scores = lax.dot_general(row_normed, col_normed, (((1,), (1,)), ((), ())), preferred_element_type=jnp.float32)
    masked = jnp.where(col_ids[None, :] < row_ids[:, None], scores, jnp.float32(-2.0))
    return lax.optimization_barrier(jnp.max(masked, axis=1))

def reference(embeds, doc_ids, prior_max, owned, owned_ids, owner_dest):
    normed = normalize(embeds).reshape(N_GRP, N_BLK, ROWS_DEV, E)
    numbers = doc_ids.reshape(N_GRP, N_BLK, ROWS_DEV)
    running = prior_max.reshape(N_GRP, N_BLK, ROWS_DEV).astype(jnp.float32)
    for distance in range(CYCLE + 1):
        col_normed = jnp.roll(normed, distance, axis=1)
        col_ids = jnp.roll(numbers, distance, axis=1)
        found = lax.map(tile_max, (normed.reshape(-1, ROWS_DEV, E), numbers.reshape(-1, ROWS_DEV), col_normed.reshape(-1, ROWS_DEV, E), col_ids.reshape(-1, ROWS_DEV)))
        running = jnp.maximum(running, found.reshape(N_GRP, N_BLK, ROWS_DEV))
    running_max = running.reshape(N_GRP, CR)
    devices = N_GRP * N_BLK
    owned_normed = normalize(owned)
    target = owner_dest[:, 0].astype(jnp.int32)
    grouped = target.reshape(devices, OWN_DEV)
    onehot = (grouped[:, :, None] == jnp.arange(devices, dtype=jnp.int32)[None, None, :]).astype(jnp.int32)
    position = lax.optimization_barrier(jnp.sum(jnp.cumsum(onehot, axis=1) * onehot, axis=2)) - 1
    source = jnp.arange(devices, dtype=jnp.int32)[:, None]
    place = (grouped * SLOTS + source * CAP + position).reshape(-1).astype(jnp.int32)
    next_rows = jnp.zeros((devices * SLOTS, E), jnp.bfloat16).at[place].set(owned_normed)
    next_ids = jnp.full((devices * SLOTS,), -1, jnp.int32).at[place].set(owned_ids.astype(jnp.int32))
    return (running_max, next_rows, next_ids)
```

```python
import functools

import jax
import jax.numpy as jnp
from jax import lax
from jax.experimental import pallas as pl
from jax.experimental.pallas import tpu as pltpu
from jax.sharding import PartitionSpec as P

CYCLE = 3
CAP = 4
CHUNKS = 4
LANES = 128
EMPTY = -2.0


def make_plan(nz):
    if nz == 4:
        received = [[], [(0, 0)], [(1, 1), (0, 1), (3, 3)], [(1, 2), (0, 2)]]
        late = [z == 3 for z in range(nz)]
    else:
        received = [[((z - 1) % nz, (z - 1) % nz), ((z - 2) % nz, (z - 1) % nz)] for z in range(nz)]
        late = [False] * nz
    own_to = [(-1, 0)] * nz
    forward = [[(-1, 0)] * len(received[z]) for z in range(nz)]
    rank = [[0] * len(received[z]) for z in range(nz)]
    returns = [0] * nz
    for z in range(nz):
        for slot, (block, source) in enumerate(received[z]):
            if block == source:
                own_to[source] = (z, slot)
            else:
                held = [entry[0] for entry in received[source]].index(block)
                forward[source][held] = (z, slot)
            rank[z][slot] = returns[block]
            returns[block] += 1
    return received, own_to, late, forward, rank, returns


def pick(index, values):
    result = jnp.int32(values[0])
    for i in range(1, len(values)):
        if values[i] != values[0]:
            result = jnp.where(index == i, jnp.int32(values[i]), result)
    return result


def kernel(plan, sizes, emb, ids, prior, owned, owned_ids, dest,
           run_out, rows_out, ids_out,
           raw, nrm, idv, idt, acc, ret, obuf, oid,
           local_sem, send_sem, recv_sem, ids_send, ids_recv, ret_send, ret_recv,
           rows_send, rows_recv, oids_send, oids_recv, keep_sem):
    n_grp, n_blk = sizes
    devices = n_grp * n_blk
    nz = n_blk // 2
    received, own_to, late, forward, rank, returns = plan
    slots = max(len(entry) for entry in received)
    rows = emb.shape[1]
    ch = rows // CHUNKS
    g = lax.axis_index("grp")
    b = lax.axis_index("blk")
    flip = g % 2
    z = b // 2
    x = b % 2
    role = z + flip * (nz - 1 - 2 * z)

    def block_of(zr):
        return 2 * (zr + flip * (nz - 1 - 2 * zr)) + x

    partner = b + 1 - 2 * x

    def table(values, slot=None, empty=0):
        if slot is None:
            return pick(role, values)
        return pick(role, [v[slot] if slot < len(v) else empty for v in values])

    own_z, own_slot = table([v[0] for v in own_to]), table([v[1] for v in own_to])
    is_late = table([int(v) for v in late])
    exists = [table([[1] * len(v) for v in received], s) for s in range(slots)]
    slot_z = [table([[e[0] for e in v] for v in received], s) for s in range(slots)]
    fwd_z = [table([[e[0] for e in v] for v in forward], s, -1) for s in range(slots)]
    fwd_slot = [table([[e[1] for e in v] for v in forward], s) for s in range(slots)]
    ranks = [table(rank, s) for s in range(slots)]
    n_returns = table(returns)
    blocks = [b, partner] + [block_of(slot_z[s]) for s in range(slots)]

    def span(c):
        if isinstance(c, int):
            return pl.ds(c * ch, ch)
        return pl.ds(pl.multiple_of(c * ch, ch), ch)

    def remote(src, dst, ssem, rsem, blk, grp=None):
        return pltpu.make_async_remote_copy(
            src_ref=src, dst_ref=dst, send_sem=ssem, recv_sem=rsem,
            device_id=(g if grp is None else grp, blk), device_id_type=pl.DeviceIdType.MESH)

    def chunk_copy(src, lane, to_slot, blk, c):
        return remote(src, raw.at[to_slot, span(c), :], send_sem.at[lane, c], recv_sem.at[to_slot, c], blk)

    def ids_copy(src, lane, to_slot, blk):
        return remote(src, idv.at[to_slot], ids_send.at[lane], ids_recv.at[to_slot], blk)

    def own_column(c):
        return chunk_copy(emb.at[0, span(c), :], 1, 2 + own_slot, block_of(own_z), c)

    def partner_copy(c):
        return chunk_copy(emb.at[0, span(c), :], 0, 1, partner, c)

    def forward_copy(s, c):
        return chunk_copy(raw.at[2 + s, span(c), :], 2 + s, 2 + fwd_slot[s], block_of(fwd_z[s]), c)

    def start_own_column():
        ids_copy(ids, 1, 2 + own_slot, block_of(own_z)).start()
        for c in range(CHUNKS):
            own_column(c).start()

    local = pltpu.make_async_copy(emb.at[0], raw.at[0], local_sem)
    local.start()

    @pl.when((own_z >= 0) & (is_late == 0))
    def _():
        start_own_column()

    ids_copy(ids, 0, 1, partner).start()
    for c in range(CHUNKS):
        partner_copy(c).start()

    def normalize(values):
        values = values.astype(jnp.float32)
        scale = lax.rsqrt(jnp.sum(values * values, axis=-1, keepdims=True) + 1e-06)
        return (values * scale).astype(jnp.bfloat16)

    own_dev = owned.shape[0]
    owned_normed = normalize(owned[...])
    t_col = dest[...].astype(jnp.float32)
    t_row = jnp.transpose(jnp.broadcast_to(t_col, (own_dev, LANES)))[0:1, :]
    row_i = lax.broadcasted_iota(jnp.int32, (own_dev, own_dev), 0)
    col_i = lax.broadcasted_iota(jnp.int32, (own_dev, own_dev), 1)
    earlier = jnp.where((row_i < col_i) & (t_col == t_row), 1.0, 0.0)
    position = jnp.sum(earlier, axis=0, keepdims=True)
    place = t_row * CAP + position
    which = lax.broadcasted_iota(jnp.int32, (devices * CAP, own_dev), 0).astype(jnp.float32)
    onehot = jnp.where(which == place, 1.0, 0.0).astype(jnp.bfloat16)
    outgoing = jnp.dot(onehot, owned_normed, preferred_element_type=jnp.float32).astype(jnp.bfloat16)
    dev_i = lax.broadcasted_iota(jnp.int32, (devices, own_dev), 0).astype(jnp.float32)
    lane_i = lax.broadcasted_iota(jnp.int32, (devices, LANES), 1)
    number = owned_ids[...].astype(jnp.float32) + 1.0
    outgoing_ids = jnp.full((devices, LANES), -1.0, jnp.float32)
    for k in range(CAP):
        here = jnp.where((dev_i == t_row) & (position == float(k)), number, 0.0)
        found = jnp.sum(here, axis=1, keepdims=True) - 1.0
        outgoing_ids = jnp.where(lane_i == k, found, outgoing_ids)
    outgoing_ids = outgoing_ids.astype(jnp.int32)
    for d in range(devices):
        obuf[d] = outgoing[d * CAP:(d + 1) * CAP, :]
        oid[d] = outgoing_ids[d:d + 1, :]

    def ready(s, c):
        at = span(c)
        nrm[s, at, :] = normalize(raw[s, at, :])
        for p in range(ch // LANES):
            at = pl.ds(pl.multiple_of(c * ch + p * LANES, LANES), LANES)
            line = idv[s, :, at].astype(jnp.float32)
            idt[s, at, :] = jnp.transpose(jnp.broadcast_to(line, (LANES, LANES)))

    def tile(row, row_at, width, col, col_at):
        scores = lax.dot_general(
            nrm[col, col_at, :], nrm[row, row_at, :], (((1,), (1,)), ((), ())),
            preferred_element_type=jnp.float32)
        row_ids = idv[row, :, row_at].astype(jnp.float32)
        col_ids = idt[col, col_at, :]
        parts = []
        for p in range(width // LANES):
            cut = slice(p * LANES, (p + 1) * LANES)
            masked = jnp.where(col_ids < row_ids[:, cut], scores[:, cut], EMPTY)
            parts.append(jnp.max(masked, axis=0, keepdims=True))
        acc[row, :, row_at] = jnp.maximum(acc[row, :, row_at], jnp.concatenate(parts, axis=1))

    whole = pl.ds(0, rows)

    acc[0] = prior[...]
    for s in range(1, 2 + slots):
        acc[s] = jnp.full((1, rows), EMPTY, jnp.float32)
    idv[0] = ids[...]
    local.wait()

    @pl.loop(0, CHUNKS)
    def _(c):
        ready(0, c)

    me = g * n_blk + b

    def to_device(step):
        other = (me + step) % devices
        return other, other // n_blk, other % n_blk

    @pl.loop(1, devices)
    def _(step):
        other, og, ob = to_device(step)
        remote(obuf.at[other], rows_out.at[me], rows_send, rows_recv, ob, og).start()
        remote(oid.at[other], ids_out.at[me], oids_send, oids_recv, ob, og).start()

    keep_rows = pltpu.make_async_copy(obuf.at[me], rows_out.at[me], keep_sem.at[0])
    keep_ids = pltpu.make_async_copy(oid.at[me], ids_out.at[me], keep_sem.at[1])
    keep_rows.start()
    keep_ids.start()

    def is_row(u, v):
        diff = (u - v + n_blk) % n_blk
        return (diff >= 1) & (diff <= CYCLE)

    def against_whole(s, c, other):
        @pl.when(is_row(blocks[s], blocks[other]))
        def _():
            tile(s, span(c), ch, other, whole)

        @pl.when(is_row(blocks[other], blocks[s]))
        def _():
            tile(other, whole, rows, s, span(c))

    def against_part(s, c, other, count):
        @pl.when(is_row(blocks[s], blocks[other]))
        def _():
            @pl.loop(0, count)
            def _(j):
                tile(s, span(c), ch, other, span(j))

        @pl.when(is_row(blocks[other], blocks[s]))
        def _():
            @pl.loop(0, count)
            def _(j):
                tile(other, span(j), ch, s, span(c))

    def arrive(s, c):
        chunk_copy(raw.at[s, span(c), :], 0, s, partner, c).wait_recv()

        @pl.when(c == 0)
        def _():
            ids_copy(idv.at[s], 0, s, partner).wait_recv()

        if s >= 2:
            @pl.when(fwd_z[s - 2] >= 0)
            def _():
                forward_copy(s - 2, c).start()

                @pl.when(c == 0)
                def _():
                    ids_copy(idv.at[s], s, 2 + fwd_slot[s - 2], block_of(fwd_z[s - 2])).start()

    @pl.loop(0, CHUNKS)
    def _(c):
        tile(0, whole, rows, 0, span(c))

    @pl.loop(0, CHUNKS)
    def _(c):
        @pl.when(exists[0] == 1)
        def _():
            arrive(2, c)
            ready(2, c)
            against_whole(2, c, 0)

    @pl.when((own_z >= 0) & (is_late == 1))
    def _():
        start_own_column()

    @pl.loop(0, CHUNKS)
    def _(c):
        for s in range(1, slots):
            @pl.when(exists[s] == 1)
            def _(s=s):
                arrive(2 + s, c)
                ready(2 + s, c)
                against_whole(2 + s, c, 0)
                against_part(2 + s, c, 1, c)

        arrive(1, c)
        ready(1, c)

        @pl.when(is_row(b, partner))
        def _():
            tile(0, whole, rows, 1, span(c))

        @pl.when(exists[0] == 1)
        def _():
            against_whole(1, c, 2)

        for s in range(1, slots):
            @pl.when(exists[s] == 1)
            def _(s=s):
                against_part(1, c, 2 + s, c + 1)

    back = remote(acc.at[1], ret.at[0], ret_send.at[0], ret_recv.at[0], partner)
    back.start()
    for s in range(slots):
        @pl.when(exists[s] == 1)
        def _(s=s):
            remote(acc.at[2 + s], ret.at[1 + ranks[s]], ret_send.at[1 + s], ret_recv.at[1 + ranks[s]],
                   block_of(slot_z[s])).start()

    for c in range(CHUNKS):
        partner_copy(c).wait_send()
    ids_copy(ids, 0, 1, partner).wait_send()

    @pl.when(own_z >= 0)
    def _():
        for c in range(CHUNKS):
            own_column(c).wait_send()
        ids_copy(ids, 1, 2 + own_slot, block_of(own_z)).wait_send()

    for s in range(slots):
        @pl.when(fwd_z[s] >= 0)
        def _(s=s):
            for c in range(CHUNKS):
                forward_copy(s, c).wait_send()
            ids_copy(idv.at[2 + s], 2 + s, 2 + fwd_slot[s], block_of(fwd_z[s])).wait_send()

    keep_rows.wait()
    keep_ids.wait()
    others = pl.ds(0, devices - 1)
    pltpu.make_async_copy(obuf.at[others], rows_out.at[others], rows_send).wait()
    pltpu.make_async_copy(oid.at[others], ids_out.at[others], oids_send).wait()
    pltpu.make_async_copy(obuf.at[others], rows_out.at[others], rows_recv).wait()
    pltpu.make_async_copy(oid.at[others], ids_out.at[others], oids_recv).wait()

    back.wait_recv()
    run_out[...] = jnp.maximum(acc[0], ret[0])
    for k in range(max(returns)):
        @pl.when(k < n_returns)
        def _(k=k):
            remote(acc.at[1], ret.at[1 + k], ret_send.at[0], ret_recv.at[1 + k], partner).wait_recv()
            run_out[...] = jnp.maximum(run_out[...], ret[1 + k])

    back.wait_send()
    for s in range(slots):
        @pl.when(exists[s] == 1)
        def _(s=s):
            remote(acc.at[2 + s], ret.at[1 + ranks[s]], ret_send.at[1 + s], ret_recv.at[1 + ranks[s]],
                   block_of(slot_z[s])).wait_send()


def body(embeds, doc_ids, prior_max, owned, owned_ids, owner_dest):
    n_grp, n_blk = lax.axis_size("grp"), lax.axis_size("blk")
    devices = n_grp * n_blk
    plan = make_plan(n_blk // 2)
    received, returns = plan[0], plan[5]
    slots = max(len(entry) for entry in received)
    rows, width = embeds.shape[1:]
    own_dev = owned.shape[0]
    vmem = pl.BlockSpec(memory_space=pltpu.VMEM)
    anywhere = pl.BlockSpec(memory_space=pl.ANY)
    dma = pltpu.SemaphoreType.DMA
    running, next_rows, next_ids = pl.pallas_call(
        functools.partial(kernel, plan, (n_grp, n_blk)),
        out_shape=(
            jax.ShapeDtypeStruct((1, rows), jnp.float32),
            jax.ShapeDtypeStruct((devices, CAP, width), jnp.bfloat16),
            jax.ShapeDtypeStruct((devices, 1, LANES), jnp.int32),
        ),
        in_specs=[anywhere, vmem, vmem, vmem, vmem, vmem],
        out_specs=(vmem, anywhere, anywhere),
        scratch_shapes=[
            pltpu.VMEM((2 + slots, rows, width), jnp.bfloat16),
            pltpu.VMEM((2 + slots, rows, width), jnp.bfloat16),
            pltpu.VMEM((2 + slots, 1, rows), jnp.int32),
            pltpu.VMEM((2 + slots, rows, LANES), jnp.float32),
            pltpu.VMEM((2 + slots, 1, rows), jnp.float32),
            pltpu.VMEM((1 + max(returns), 1, rows), jnp.float32),
            pltpu.VMEM((devices, CAP, width), jnp.bfloat16),
            pltpu.VMEM((devices, 1, LANES), jnp.int32),
            dma, dma((2 + slots, CHUNKS)), dma((2 + slots, CHUNKS)),
            dma((2 + slots,)), dma((2 + slots,)),
            dma((1 + slots,)), dma((1 + max(returns),)),
            dma, dma, dma, dma, dma((2,)),
        ],
        compiler_params=pltpu.CompilerParams(has_side_effects=True, vmem_limit_bytes=60 * 1024 * 1024),
    )(embeds, doc_ids, prior_max, owned, owned_ids.reshape(1, own_dev), owner_dest)
    return (running, next_rows.reshape(devices * CAP, width), next_ids[:, 0, :CAP].reshape(devices * CAP))


def solution(mesh):
    return jax.shard_map(
        body,
        mesh=mesh,
        in_specs=(
            P("grp", "blk", None),
            P("grp", "blk"),
            P("grp", "blk"),
            P(("grp", "blk"), None),
            P(("grp", "blk")),
            P(("grp", "blk"), None),
        ),
        out_specs=(P("grp", "blk"), P(("grp", "blk"), None), P(("grp", "blk"))),
        check_vma=False,
    )
```
